16 devices in a mesh: rep: 2 (over y, z), dp: 8 (over x, core).
Axes of the slice: x: 4, y: 2, z: 1, core: 2. Of those that a mesh axis runs over, the one named last changes fastest.
The devices are a block of a 4x4x8 slice.
Arguments:
- x: bfloat16 [16, 2048, 896], P(('rep', 'dp')), parts along dimension 0
- dy: bfloat16 [16, 2048, 896], P(('rep', 'dp')), parts along dimension 0
- wq: bfloat16 [2, 896, 896], P(None, 'dp')
- wk: bfloat16 [2, 896, 128], P(None, 'dp')
- wv: bfloat16 [2, 896, 128], P(None, 'dp')
- wo: bfloat16 [2, 896, 896], P(None, 'dp')
- w_gate: bfloat16 [2, 896, 2560], P(None, 'dp')
- w_up: bfloat16 [2, 896, 2560], P(None, 'dp')
- w_down: bfloat16 [2, 2560, 896], P(None, 'dp')
Outputs:
- output 1: bfloat16 [16, 2048, 896], P(('rep', 'dp')), parts along dimension 0
- output 2: bfloat16 [4, 896, 896], P('rep', 'dp'), parts along dimension 0
- output 3: bfloat16 [4, 896, 128], P('rep', 'dp'), parts along dimension 0
- output 4: bfloat16 [4, 896, 128], P('rep', 'dp'), parts along dimension 0
- output 5: bfloat16 [4, 896, 896], P('rep', 'dp'), parts along dimension 0
- output 6: bfloat16 [4, 896, 2560], P('rep', 'dp'), parts along dimension 0
- output 7: bfloat16 [4, 896, 2560], P('rep', 'dp'), parts along dimension 0
- output 8: bfloat16 [4, 2560, 896], P('rep', 'dp'), parts along dimension 0
There are 2 independent parts. The reference program is written for one: setup_inputs(seed, part) draws one part's arguments, and reference() takes and returns one part's arrays. A program takes and returns all parts, laid end to end along the dimension named above; an argument that names none is the same for every part.
All inputs are finite; a program needn't handle non-finite values.
Results may differ from the reference program's by a relative error of at most 0.0286.
Values are sent between devices in bfloat16 or wider.
A program may use at most 768 MiB of HBM per device.

```python
import jax
import jax.numpy as jnp
from jax import lax

SEQUENCES = 8
TOKENS = 2048
D = 896
HEADS = 7
KV_HEADS = 1
HEAD = 128
FF = 2560
LAYERS = 2
THETA = 10000
NAMES = ("wq", "wk", "wv", "wo", "w_gate", "w_up", "w_down")
SHAPES = {
    "wq": (LAYERS, D, HEADS * HEAD),
    "wk": (LAYERS, D, KV_HEADS * HEAD),
    "wv": (LAYERS, D, KV_HEADS * HEAD),
    "wo": (LAYERS, HEADS * HEAD, D),
    "w_gate": (LAYERS, D, FF),
    "w_up": (LAYERS, D, FF),
    "w_down": (LAYERS, FF, D),
}


def bump(key, n, height):
    away = (jnp.arange(n, dtype=jnp.int32) - jax.random.randint(key, (), 0, n, jnp.int32)) % n
    return jnp.where(away < n // 8, height, 1.0)


def together(key, own, strength):
    shared = jax.random.normal(key, own.shape[1:], jnp.float32)
    return (own + strength * shared) * lax.rsqrt(1 + strength * strength)


def setup_inputs(seed: int = 0, part: int = 0) -> dict:
    kx, kdy, ka, kb, kz, kf, kh, kl, *keys = jax.random.split(jax.random.key(seed), 8 + 3 * len(NAMES))
    kx, kdy, ka, kb = (jax.random.fold_in(k, part) for k in (kx, kdy, ka, kb))
    kw, km, kv = (keys[i::3] for i in range(3))
    shape = (SEQUENCES, TOKENS, D)
    much_x, much_dy = jax.random.uniform(kz, (2,), jnp.float32, 0.0, 1.0)
    loud = 2.0 ** jax.random.uniform(jax.random.fold_in(kz, 1), (), jnp.float32, -1.0, 2.0)
    layers = 2.0 ** jax.random.uniform(kl, (LAYERS, 1, 1), jnp.float32, -1.0, 1.0)
    times = {"wq": 1.0, "wk": 1.0, "wv": 2.0, "wo": layers, "w_gate": 1.0, "w_up": bump(kh, FF, 4.0), "w_down": layers}
    x = together(ka, jax.random.normal(kx, shape, jnp.float32), much_x) * bump(kf, D, 4.0)
    dy = together(kb, jax.random.normal(kdy, shape, jnp.float32), much_dy)
    drawn = {"x": x.astype(jnp.bfloat16), "dy": (loud * dy * (SEQUENCES * TOKENS) ** -0.5).astype(jnp.bfloat16)}
    for key, name in zip(kw, NAMES, strict=True):
        drawn[name] = (jax.random.normal(key, SHAPES[name], jnp.float32) * SHAPES[name][1] ** -0.5 * times[name]).astype(jnp.bfloat16)
    return drawn


def matmul(a, w):
    return jnp.dot(a, w, preferred_element_type=jnp.float32).astype(jnp.bfloat16)


def normed(h):
    wide = h.astype(jnp.float32)
    scale = lax.rsqrt(jnp.mean(wide**2, -1, keepdims=True) + 1e-6)
    return (wide * scale).astype(jnp.bfloat16)


def turned(t, theta):
    half = t.shape[-1] // 2
    angle = jnp.arange(t.shape[0], dtype=jnp.float32)[:, None] * theta ** (-jnp.arange(half, dtype=jnp.float32) / half)
    cos, sin = jnp.cos(angle)[:, None], jnp.sin(angle)[:, None]
    a, b = t[..., :half].astype(jnp.float32), t[..., half:].astype(jnp.float32)
    return jnp.concatenate([a * cos - b * sin, b * cos + a * sin], -1).astype(jnp.bfloat16)


def seen_by(q, k, v):
    tokens, kv = q.shape[0], k.shape[1]
    q = q.reshape(tokens, kv, -1, q.shape[-1])
    scores = jnp.einsum("tgsd,ugd->gstu", q.astype(jnp.float32), k.astype(jnp.float32)) * q.shape[-1] ** -0.5
    place = jnp.arange(tokens)
    weights = jax.nn.softmax(jnp.where(place[:, None] >= place, scores, -jnp.inf), -1).astype(jnp.bfloat16)
    return jnp.einsum("gstu,ugd->tgsd", weights.astype(jnp.float32), v.astype(jnp.float32)).astype(jnp.bfloat16).reshape(tokens, -1)


def layer(h, w):
    a = normed(h)
    q, k = (turned(matmul(a, w[name]).reshape(h.shape[0], -1, HEAD), THETA) for name in ("wq", "wk"))
    h = h + matmul(seen_by(q, k, matmul(a, w["wv"]).reshape(h.shape[0], -1, HEAD)), w["wo"])
    b = normed(h)
    gate = jnp.dot(b, w["w_gate"], preferred_element_type=jnp.float32)
    up = jnp.dot(b, w["w_up"], preferred_element_type=jnp.float32)
    return h + matmul((jax.nn.silu(gate) * up).astype(jnp.bfloat16), w["w_down"])


def stack(weights, h):
    return lax.scan(lambda h, w: (layer(h, w), None), h, weights)[0]


def reference(x, dy, wq, wk, wv, wo, w_gate, w_up, w_down):
    weights = dict(zip(NAMES, (wq, wk, wv, wo, w_gate, w_up, w_down), strict=True))

    def take(so_far, sequence):
        h, by_y = sequence
        _, back = jax.vjp(stack, weights, h)
        by_weights, by_h = back(by_y)
        return jax.tree.map(lambda total, term: total + term.astype(jnp.float32), so_far, by_weights), by_h

    none_yet = {name: jnp.zeros(w.shape, jnp.float32) for name, w in weights.items()}
    by_weights, by_x = lax.scan(take, none_yet, (x, dy))
    return (by_x, *(by_weights[name].astype(jnp.bfloat16) for name in NAMES))
```

```python
import functools

import jax
import jax.numpy as jnp
from jax import lax
from jax.experimental import pallas as pl
from jax.experimental.pallas import tpu as pltpu
from jax.sharding import PartitionSpec as P

HEAD = 128
THETA = 10000
NEG = -1e30
HIDDEN = 2 * NEG
LOG2E = 1.4426950408889634
LOW, WIDE = jnp.bfloat16, jnp.float32
VMEM = 60 * 2**20
SCALE = HEAD**-0.5


def _fit(size, want, unit=128):
    return max(n for n in range(unit, max(min(want, size), unit) + 1, unit) if size % n == 0)


def _dot(a, b, ca=1, cb=0):
    return lax.dot_general(a, b, (((ca,), (cb,)), ((), ())), preferred_element_type=WIDE)


def _call(kernel, grid, ins, in_specs, outs, out_specs, scratch=(), flops=0, exps=0, order=None):
    size = sum(a.size * a.dtype.itemsize for a in [*ins, *outs])
    body = kernel.func if isinstance(kernel, functools.partial) else kernel
    return pl.pallas_call(
        kernel,
        name=body.__name__.strip("_"),
        grid=grid,
        in_specs=in_specs,
        out_specs=out_specs,
        out_shape=outs,
        scratch_shapes=list(scratch),
        compiler_params=pltpu.CompilerParams(dimension_semantics=order or ("arbitrary",) * len(grid), vmem_limit_bytes=VMEM),
        cost_estimate=pl.CostEstimate(flops=flops, transcendentals=exps, bytes_accessed=size),
    )(*ins)


def _whole(a):
    return pl.BlockSpec(a.shape, lambda *_: (0,) * a.ndim, pipeline_mode=pl.Buffered(1))


def _rows(tm, width):
    return pl.BlockSpec((tm, width), lambda i, *_: (i, 0))


def _new(shape, dtype=LOW):
    return jax.ShapeDtypeStruct(shape, dtype)


def _scale_of(wide):
    return lax.rsqrt(jnp.mean(wide**2, -1, keepdims=True) + 1e-6)


def _normed(h):
    wide = h.astype(WIDE)
    return (wide * _scale_of(wide)).astype(LOW)


def _norm_back(h, d_out):
    wide = h.astype(WIDE)
    scale = _scale_of(wide)
    along = jnp.sum(d_out * wide, -1, keepdims=True) / wide.shape[-1]
    return scale * d_out - wide * (scale * scale * scale * along)


def _angles(tokens):
    half = HEAD // 2
    angle = jnp.arange(tokens, dtype=WIDE)[:, None] * THETA ** (-jnp.arange(half, dtype=WIDE) / half)
    cos, sin = jnp.cos(angle), jnp.sin(angle)
    return jnp.concatenate([cos, cos], 1), jnp.concatenate([-sin, sin], 1)


def _turned(t, cos, sin):
    return (t * cos + pltpu.roll(t, HEAD // 2, 1) * sin).astype(LOW)


def _qkv_kernel(h_ref, w_ref, cos_ref, sin_ref, a_ref, q_ref, k_ref, v_ref, *, at):
    heads = q_ref.shape[0]
    a = _normed(h_ref[...])
    a_ref[...] = a
    t = _dot(a, w_ref[:, at:]).astype(LOW)
    cos, sin = cos_ref[...], sin_ref[...]
    for n in range(heads):
        q_ref[n] = _turned(t[:, n * HEAD : (n + 1) * HEAD].astype(WIDE), cos, sin)
    k_ref[...] = _turned(t[:, heads * HEAD : (heads + 1) * HEAD].astype(WIDE), cos, sin)
    v_ref[...] = t[:, (heads + 1) * HEAD :]


def qkv(h, w, cos, sin, at):
    tokens, d = h.shape
    heads = (w.shape[1] - at) // HEAD - 2
    tm = _fit(tokens, 512)
    row = _rows(tm, HEAD)
    return _call(
        functools.partial(_qkv_kernel, at=at), (tokens // tm,), [h, w, cos, sin], [_rows(tm, d), _whole(w), row, row],
        [_new((tokens, d)), _new((heads, tokens, HEAD)), _new((tokens, HEAD)), _new((tokens, HEAD))],
        [_rows(tm, d), pl.BlockSpec((heads, tm, HEAD), lambda i: (0, i, 0)), row, row],
        flops=2 * tokens * d * (heads + 2) * HEAD,
    )


def _gap(bk, cols, bq):
    return lax.rem(lax.broadcasted_iota(jnp.int32, (bk, cols), 1), bq) - lax.broadcasted_iota(jnp.int32, (bk, cols), 0)


def _lanes(ref):
    return jnp.concatenate([ref[n : n + 1, :] for n in range(ref.shape[0])], axis=1)


def _attend_kernel(q_ref, k_ref, v_ref, o_ref, lse_ref, top_s, mix_s, gap_s, *, bq, bk, wide):
    g = q_ref.shape[0]
    cols = g * bq
    iq = pl.program_id(0)
    e = SCALE * LOG2E
    pieces = list(range(0, cols, wide))

    @pl.when(iq == 0)
    def _():
        gap_s[...] = _gap(bk, cols, bq)

    top_s[...] = jnp.full(top_s.shape, NEG, WIDE)
    mix_s[...] = jnp.zeros(mix_s.shape, WIDE)
    ones = jnp.ones((8, bk), LOW)

    def block(j, masked):
        here = pl.ds(pl.multiple_of(j * bk, bk), bk)
        q = q_ref[...].reshape(cols, HEAD)
        scores = [_dot(k_ref[here, :], q[at : at + wide, :], 1, 1) for at in pieces]
        if masked:
            ok = gap_s[...] >= j * bk - iq * bq
        values = jnp.concatenate([v_ref[here, :].T, ones], axis=0)
        weights, keeps = [], []
        for at, s in zip(pieces, scores):
            if masked:
                s = jnp.where(ok[:, at : at + wide], s, HIDDEN)
            old = top_s[:, at : at + wide]
            top = jnp.maximum(old, s.max(axis=0, keepdims=True))
            top_s[:, at : at + wide] = top
            weights.append(jnp.exp2((s - top) * e).astype(LOW))
            keeps.append(jnp.exp2((old - top) * e))
        for at, p, keep in zip(pieces, weights, keeps):
            mix_s[:, at : at + wide] = mix_s[:, at : at + wide] * keep + _dot(values, p, 1, 0)

    whole, last = lax.div(iq * bq + 1, bk), lax.div(iq * bq + bq - 1 + bk, bk)
    lax.fori_loop(0, whole, lambda j, _: block(j, False), None)
    lax.fori_loop(whole, last, lambda j, _: block(j, True), None)
    total = mix_s[HEAD : HEAD + 1, :]
    out = mix_s[:HEAD, :] * (1 / total)
    lse = top_s[...] * SCALE + jnp.log(total)
    for n in range(g):
        o_ref[:, n * HEAD : (n + 1) * HEAD] = out[:, n * bq : (n + 1) * bq].T.astype(o_ref.dtype)
        lse_ref[n : n + 1, :] = lse[:, n * bq : (n + 1) * bq]


def attend(q, k, v, bq=512, bk=512, wide=512):
    g, tokens, _ = q.shape
    bq, bk = _fit(tokens, bq), _fit(tokens, bk)
    wide = _fit(g * bq, wide)
    return _call(
        functools.partial(_attend_kernel, bq=bq, bk=bk, wide=wide), (tokens // bq,), [q, k, v],
        [pl.BlockSpec((g, bq, HEAD), lambda i: (0, i, 0)), _whole(k), _whole(v)],
        [_new((tokens, g * HEAD)), _new((g, tokens), WIDE)],
        [_rows(bq, g * HEAD), pl.BlockSpec((g, bq), lambda i: (0, i))],
        [pltpu.VMEM((1, g * bq), WIDE), pltpu.VMEM((HEAD + 8, g * bq), WIDE), pltpu.VMEM((bk, g * bq), jnp.int32)],
        flops=4 * g * tokens * tokens * HEAD, exps=g * tokens * tokens,
    )


def _wo_kernel(o_ref, w_ref, h_ref, h2_ref, b_ref):
    d = h_ref.shape[1]
    h2 = (h_ref[...].astype(WIDE) + _dot(o_ref[...], w_ref[:, :d]).astype(LOW).astype(WIDE)).astype(LOW)
    h2_ref[...] = h2
    b_ref[...] = _normed(h2)


def out_project(o, w, h):
    tokens, d = h.shape
    tm = _fit(tokens, 512)
    return _call(
        _wo_kernel, (tokens // tm,), [o, w, h], [_rows(tm, o.shape[1]), _whole(w), _rows(tm, d)],
        [_new((tokens, d)), _new((tokens, d))], [_rows(tm, d), _rows(tm, d)], flops=2 * tokens * d * o.shape[1],
    )


def _gate_up_kernel(b_ref, wg_ref, wu_ref, g_ref, u_ref, act_ref):
    b = b_ref[...]
    g, u = _dot(b, wg_ref[...]), _dot(b, wu_ref[...])
    g_ref[...] = g
    u_ref[...] = u
    act_ref[...] = (g * lax.logistic(g) * u).astype(LOW)


def gate_up(b, w, tm=1024, tf=512):
    tokens, d = b.shape
    ff = w.shape[1] // 2
    tm, tf = _fit(tokens, tm), _fit(ff, tf)
    per = ff // tf
    tile = pl.BlockSpec((tm, tf), lambda i, j: (i, j))
    return _call(
        _gate_up_kernel, (tokens // tm, per), [b, w, w],
        [_rows(tm, d), pl.BlockSpec((d, tf), lambda i, j: (0, j)), pl.BlockSpec((d, tf), lambda i, j: (0, j + per))],
        [_new((tokens, ff), WIDE), _new((tokens, ff), WIDE), _new((tokens, ff))], [tile] * 3,
        flops=4 * tokens * d * ff, exps=tokens * ff,
    )


def _down_kernel(act_ref, w_ref, h_ref, y_ref):
    y_ref[...] = (h_ref[...].astype(WIDE) + _dot(act_ref[...], w_ref[...]).astype(LOW).astype(WIDE)).astype(LOW)


def down(act, w, h):
    tokens, d = h.shape
    tm = _fit(tokens, 512)
    return _call(
        _down_kernel, (tokens // tm,), [act, w, h], [_rows(tm, act.shape[1]), _whole(w), _rows(tm, d)],
        [_new((tokens, d))], [_rows(tm, d)], flops=2 * tokens * d * act.shape[1],
    )[0]


def _mlp_back_kernel(*refs, kept):
    if kept:
        dy_ref, h2_ref, wg_ref, wu_ref, wd_ref, g_ref, u_ref, dgu_ref, dh_ref, db_s = refs
        g, u = g_ref[...], u_ref[...]
    else:
        dy_ref, h2_ref, wg_ref, wu_ref, wd_ref, b_ref, dgu_ref, dh_ref, act_ref, db_s = refs
        b = b_ref[...]
        g, u = _dot(b, wg_ref[...]), _dot(b, wu_ref[...])
    j = pl.program_id(1)
    d_act = _dot(dy_ref[...], wd_ref[...], 1, 1).astype(LOW).astype(WIDE)
    half = lax.logistic(g)
    silu = g * half
    if not kept:
        act_ref[...] = (silu * u).astype(LOW)
    du = (d_act * silu).astype(LOW)
    dg = (d_act * u * (half + silu * (1 - half))).astype(LOW)
    dgu_ref[0] = dg
    dgu_ref[1] = du
    term = _dot(jnp.concatenate([dg, du], 1), jnp.concatenate([wg_ref[...], wu_ref[...]], 1), 1, 1)

    @pl.when(j == 0)
    def _():
        db_s[...] = term

    @pl.when(j > 0)
    def _():
        db_s[...] += term

    @pl.when(j == pl.num_programs(1) - 1)
    def _():
        back = _norm_back(h2_ref[...], db_s[...].astype(LOW).astype(WIDE))
        dh_ref[...] = (dy_ref[...].astype(WIDE) + back).astype(LOW)


def mlp_back(dy, h2, w, w_down, b=None, kept=None, tm=1024, tf=512):
    tokens, d = dy.shape
    ff = w.shape[1] // 2
    tm, tf = _fit(tokens, tm), _fit(ff, tf)
    per = ff // tf
    tile = pl.BlockSpec((tm, tf), lambda i, j: (i, j))
    ins = [dy, h2, w, w, w_down]
    specs = [_rows(tm, d), _rows(tm, d), pl.BlockSpec((d, tf), lambda i, j: (0, j)), pl.BlockSpec((d, tf), lambda i, j: (0, j + per)),
             pl.BlockSpec((tf, d), lambda i, j: (j, 0))]
    outs = [_new((2, tokens, ff)), _new((tokens, d))]
    out_specs = [pl.BlockSpec((2, tm, tf), lambda i, j: (0, i, j)), _rows(tm, d)]
    if kept is None:
        ins, specs = [*ins, b], [*specs, _rows(tm, d)]
        outs, out_specs = [*outs, _new((tokens, ff))], [*out_specs, tile]
    else:
        ins, specs = [*ins, *kept[:2]], [*specs, tile, tile]
    got = _call(
        functools.partial(_mlp_back_kernel, kept=kept is not None), (tokens // tm, per), ins, specs, outs, out_specs,
        [pltpu.VMEM((tm, d), WIDE)], flops=(6 if kept else 10) * tokens * d * ff, exps=tokens * ff,
    )
    return got if kept is None else (*got, kept[2])


def _grad_kernel(a_ref, b_ref, c_ref, at_s, *, flip):
    @pl.when(pl.program_id(0) == 0)
    def _():
        at_s[...] = a_ref[...].T

    c = _dot(at_s[...], b_ref[0])
    c_ref[...] = (c.T if flip else c).astype(LOW)


def weight_grad(a, b, flip=False, tn=512):
    tokens, d = a.shape
    parts, _, n = b.shape
    tn = _fit(n, tn)
    per = n // tn
    total = parts * n
    return _call(
        functools.partial(_grad_kernel, flip=flip), (parts * per,), [a, b],
        [_whole(a), pl.BlockSpec((1, tokens, tn), lambda i: (lax.div(i, per), 0, lax.rem(i, per)))],
        [_new((total, d) if flip else (d, total))],
        [pl.BlockSpec((tn, d), lambda i: (i, 0)) if flip else pl.BlockSpec((d, tn), lambda i: (0, i))],
        [pltpu.VMEM((d, tokens), LOW)], flops=2 * tokens * d * total,
    )[0]


def _wo_back_kernel(dh_ref, w_ref, o_ref, do_ref, delta_ref):
    heads, d = do_ref.shape[0], dh_ref.shape[1]
    d_out = _dot(dh_ref[...], w_ref[:, :d], 1, 1).astype(LOW)
    along = d_out.astype(WIDE) * o_ref[...].astype(WIDE)
    for n in range(heads):
        at = slice(n * HEAD, (n + 1) * HEAD)
        do_ref[n] = d_out[:, at]
        delta_ref[n : n + 1, :] = jnp.sum(along[:, at].T, axis=0, keepdims=True)


def out_project_back(dh, w, o):
    tokens, d = dh.shape
    width = o.shape[1]
    heads = width // HEAD
    tm = _fit(tokens, 512)
    return _call(
        _wo_back_kernel, (tokens // tm,), [dh, w, o], [_rows(tm, d), _whole(w), _rows(tm, width)],
        [_new((heads, tokens, HEAD)), _new((heads, tokens), WIDE)],
        [pl.BlockSpec((heads, tm, HEAD), lambda i: (0, i, 0)), pl.BlockSpec((heads, tm), lambda i: (0, i))],
        flops=2 * tokens * d * width,
    )


def _attend_back_kernel(q_ref, k_ref, v_ref, do_ref, lse_ref, delta_ref, dq_ref, dk_ref, dv_ref, dq_s, dk_s, dv_s, gap_s, *, bq, bk, wide):
    g = q_ref.shape[0]
    cols = g * bq
    iq = pl.program_id(0)
    e = SCALE * LOG2E
    pieces = list(range(0, cols, wide))

    @pl.when(iq == 0)
    def _():
        gap_s[...] = _gap(bk, cols, bq)
        dk_s[...] = jnp.zeros_like(dk_s)
        dv_s[...] = jnp.zeros_like(dv_s)

    dq_s[...] = jnp.zeros_like(dq_s)
    lses = _lanes(lse_ref) * LOG2E
    deltas = _lanes(delta_ref)

    def block(j, masked):
        here = pl.ds(pl.multiple_of(j * bk, bk), bk)
        q, do = q_ref[...].reshape(cols, HEAD), do_ref[...].reshape(cols, HEAD)
        qs, dos = [q[at : at + wide, :] for at in pieces], [do[at : at + wide, :] for at in pieces]
        scores = [_dot(k_ref[here, :], x, 1, 1) for x in qs]
        dps = [_dot(v_ref[here, :], x, 1, 1) for x in dos]
        if masked:
            ok = gap_s[...] >= j * bk - iq * bq
        for n, at in enumerate(pieces):
            p = jnp.exp2(scores[n] * e - lses[:, at : at + wide])
            if masked:
                p = jnp.where(ok[:, at : at + wide], p, 0.0)
            ds = (p * (dps[n] - deltas[:, at : at + wide])).astype(LOW)
            dv_s[here, :] += _dot(p.astype(LOW), dos[n], 1, 0)
            dk_s[here, :] += _dot(ds, qs[n], 1, 0)
            dq_s[:, at : at + wide] += _dot(k_ref[here, :].T, ds, 1, 0)

    whole, last = lax.div(iq * bq + 1, bk), lax.div(iq * bq + bq - 1 + bk, bk)
    lax.fori_loop(0, whole, lambda j, _: block(j, False), None)
    lax.fori_loop(whole, last, lambda j, _: block(j, True), None)
    dq_ref[...] = (dq_s[...] * SCALE).T.reshape(g, bq, HEAD).astype(LOW)

    @pl.when(iq == pl.num_programs(0) - 1)
    def _():
        dk_ref[...] = (dk_s[...] * SCALE).astype(LOW)
        dv_ref[...] = dv_s[...].astype(LOW)


def attend_back(q, k, v, d_out, lse, delta, bq=256, bk=512, wide=512):
    g, tokens, _ = q.shape
    bq, bk = _fit(tokens, bq), _fit(tokens, bk)
    wide = _fit(g * bq, wide)
    block = pl.BlockSpec((g, bq, HEAD), lambda i: (0, i, 0))
    stats = pl.BlockSpec((g, bq), lambda i: (0, i))
    return _call(
        functools.partial(_attend_back_kernel, bq=bq, bk=bk, wide=wide), (tokens // bq,), [q, k, v, d_out, lse, delta],
        [block, _whole(k), _whole(v), block, stats, stats],
        [_new(q.shape), _new(k.shape), _new(v.shape)], [block, _whole(k), _whole(v)],
        [pltpu.VMEM((HEAD, g * bq), WIDE), pltpu.VMEM(k.shape, WIDE), pltpu.VMEM(v.shape, WIDE), pltpu.VMEM((bk, g * bq), jnp.int32)],
        flops=10 * g * tokens * tokens * HEAD, exps=g * tokens * tokens,
    )


def _qkv_back_kernel(dq_ref, dk_ref, dv_ref, cos_ref, sin_ref, w_ref, h_ref, dh2_ref, dt_ref, dh_ref, *, at):
    heads = dq_ref.shape[0]
    cos, sin = cos_ref[...], -sin_ref[...]
    for n in range(heads):
        dt_ref[:, n * HEAD : (n + 1) * HEAD] = _turned(dq_ref[n].astype(WIDE), cos, sin)
    dt_ref[:, heads * HEAD : (heads + 1) * HEAD] = _turned(dk_ref[...].astype(WIDE), cos, sin)
    dt_ref[:, (heads + 1) * HEAD :] = dv_ref[...]
    da = _dot(dt_ref[...], w_ref[:, at:], 1, 1).astype(LOW).astype(WIDE)
    dh_ref[...] = (dh2_ref[...].astype(WIDE) + _norm_back(h_ref[...], da)).astype(LOW)


def qkv_back(dq, dk, dv, cos, sin, w, h, dh2, at):
    tokens, d = h.shape
    heads = dq.shape[0]
    width = (heads + 2) * HEAD
    tm = _fit(tokens, 512)
    row = _rows(tm, HEAD)
    return _call(
        functools.partial(_qkv_back_kernel, at=at), (tokens // tm,), [dq, dk, dv, cos, sin, w, h, dh2],
        [pl.BlockSpec((heads, tm, HEAD), lambda i: (0, i, 0)), row, row, row, row, _whole(w), _rows(tm, d), _rows(tm, d)],
        [_new((tokens, width)), _new((tokens, d))], [_rows(tm, width), _rows(tm, d)], flops=2 * tokens * d * width,
    )


def solution(mesh):
    def gather(w):
        return lax.all_gather(w, "dp", axis=0, tiled=True)

    def scatter(d_w):
        return lax.psum_scatter(d_w, "dp", scatter_dimension=0, tiled=True)

    tied = lambda *arrays: lax.optimization_barrier(arrays)

    def step(x, dy, wq, wk, wv, wo, w_gate, w_up, w_down):
        layers = wq.shape[0]
        h, d_h = x[0], dy[0]
        at = wo.shape[2]
        blocks = []
        for n in range(layers):
            blocks.append((
                gather(jnp.concatenate([wo[n], wq[n], wk[n], wv[n]], 1)),
                gather(jnp.concatenate([w_gate[n], w_up[n]], 1)),
                gather(w_down[n]),
            ))
        cos, sin = _angles(h.shape[0])
        kept = []
        for n in range(layers):
            near, middle, far = blocks[n]
            a, q, k, v = qkv(h, near, cos, sin, at)
            o, lse = attend(q, k, v)
            h2, b = out_project(o, near, h)
            last = n == layers - 1
            mlp = None if last else gate_up(b, middle)
            kept.append((h, a, q, k, v, o, lse, h2, b, mlp))
            if not last:
                h = down(mlp[2], far, h2)
        mine = [None] * layers
        late = None
        for n in reversed(range(layers)):
            near, middle, far = blocks[n]
            h, a, q, k, v, o, lse, h2, b, mlp = kept[n]
            dgu, dh2, act = mlp_back(d_h, h2, middle, far, b, mlp)
            if late is not None:
                late, act, dh2 = tied(late, act, dh2)
                mine[n + 1][3] = late
            d_down, b = tied(weight_grad(d_h, act[None], flip=True), b)
            d_gu, o = tied(weight_grad(b, dgu), o)
            d_wo, dh2 = tied(weight_grad(o, dh2[None]), dh2)
            d_down, d_gu, d_wo = (scatter(t) for t in (d_down, d_gu, d_wo))
            d_out, delta = out_project_back(dh2, near, o)
            d_down, d_out = tied(d_down, d_out)
            dq, dk, dv = attend_back(q, k, v, d_out, lse, delta)
            d_gu, dq = tied(d_gu, dq)
            dt, d_h = qkv_back(dq, dk, dv, cos, sin, near, h, dh2, at)
            d_wo, dt, d_h = tied(d_wo, dt, d_h)
            d_qkv = weight_grad(a, dt[None])
            d_qkv, d_h = tied(d_qkv, d_h)
            late = scatter(d_qkv)
            mine[n] = [d_down, d_gu, d_wo, late]
        ff = w_gate.shape[2]
        qs = wq.shape[2]
        ks = qs + wk.shape[2]
        mine = [(t[:, :qs], t[:, qs:ks], t[:, ks:], d_wo, d_gu[:, :ff], d_gu[:, ff:], d_down) for d_down, d_gu, d_wo, t in mine]
        return (d_h[None], *(jnp.stack([mine[n][i] for n in range(layers)]) for i in range(7)))

    states, cut = P(("rep", "dp"), None, None), P(None, "dp", None)
    return jax.shard_map(
        step,
        mesh=mesh,
        in_specs=(states, states) + (cut,) * 7,
        out_specs=(states,) + (P("rep", "dp", None),) * 7,
        check_vma=False,
    )
```

```python
import functools

import jax
import jax.numpy as jnp
from jax import lax
from jax.experimental import pallas as pl
from jax.experimental.pallas import tpu as pltpu
from jax.sharding import PartitionSpec as P

HEAD = 128
THETA = 10000
NEG = -1e30
HIDDEN = 2 * NEG
LOG2E = 1.4426950408889634
LOW, WIDE = jnp.bfloat16, jnp.float32
VMEM = 60 * 2**20
SCALE = HEAD**-0.5


def _fit(size, want, unit=128):
    return max(n for n in range(unit, max(min(want, size), unit) + 1, unit) if size % n == 0)


def _dot(a, b, ca=1, cb=0):
    return lax.dot_general(a, b, (((ca,), (cb,)), ((), ())), preferred_element_type=WIDE)


def _call(kernel, grid, ins, in_specs, outs, out_specs, scratch=(), flops=0, exps=0, order=None):
    size = sum(a.size * a.dtype.itemsize for a in [*ins, *outs])
    body = kernel.func if isinstance(kernel, functools.partial) else kernel
    return pl.pallas_call(
        kernel,
        name=body.__name__.strip("_"),
        grid=grid,
        in_specs=in_specs,
        out_specs=out_specs,
        out_shape=outs,
        scratch_shapes=list(scratch),
        compiler_params=pltpu.CompilerParams(dimension_semantics=order or ("arbitrary",) * len(grid), vmem_limit_bytes=VMEM),
        cost_estimate=pl.CostEstimate(flops=flops, transcendentals=exps, bytes_accessed=size),
    )(*ins)


def _whole(a):
    return pl.BlockSpec(a.shape, lambda *_: (0,) * a.ndim, pipeline_mode=pl.Buffered(1))


def _left(a, width):
    return pl.BlockSpec((a.shape[0], width), lambda *_: (0, 0), pipeline_mode=pl.Buffered(1))


def _rows(tm, width):
    return pl.BlockSpec((tm, width), lambda i, *_: (i, 0))


def _new(shape, dtype=LOW):
    return jax.ShapeDtypeStruct(shape, dtype)


def _scale_of(wide):
    return lax.rsqrt(jnp.mean(wide**2, -1, keepdims=True) + 1e-6)


def _normed(h):
    wide = h.astype(WIDE)
    return (wide * _scale_of(wide)).astype(LOW)


def _norm_back(h, d_out):
    wide = h.astype(WIDE)
    scale = _scale_of(wide)
    along = jnp.sum(d_out * wide, -1, keepdims=True) / wide.shape[-1]
    return scale * d_out - wide * (scale * scale * scale * along)


def _angles(tokens):
    half = HEAD // 2
    angle = jnp.arange(tokens, dtype=WIDE)[:, None] * THETA ** (-jnp.arange(half, dtype=WIDE) / half)
    cos, sin = jnp.cos(angle), jnp.sin(angle)
    return jnp.concatenate([cos, cos], 1), jnp.concatenate([-sin, sin], 1)


def _turned(t, cos, sin):
    return (t * cos + pltpu.roll(t, HEAD // 2, 1) * sin).astype(LOW)


def _qkv_kernel(h_ref, w_ref, cos_ref, sin_ref, a_ref, q_ref, k_ref, v_ref, *, at):
    heads = q_ref.shape[0]
    a = _normed(h_ref[...])
    a_ref[...] = a
    t = _dot(a, w_ref[:, at:]).astype(LOW)
    cos, sin = cos_ref[...], sin_ref[...]
    for n in range(heads):
        q_ref[n] = _turned(t[:, n * HEAD : (n + 1) * HEAD].astype(WIDE), cos, sin)
    k_ref[...] = _turned(t[:, heads * HEAD : (heads + 1) * HEAD].astype(WIDE), cos, sin)
    v_ref[...] = t[:, (heads + 1) * HEAD :]


def qkv(h, w, cos, sin, at):
    tokens, d = h.shape
    heads = (w.shape[1] - at) // HEAD - 2
    tm = _fit(tokens, 512)
    row = _rows(tm, HEAD)
    return _call(
        functools.partial(_qkv_kernel, at=at), (tokens // tm,), [h, w, cos, sin], [_rows(tm, d), _whole(w), row, row],
        [_new((tokens, d)), _new((heads, tokens, HEAD)), _new((tokens, HEAD)), _new((tokens, HEAD))],
        [_rows(tm, d), pl.BlockSpec((heads, tm, HEAD), lambda i: (0, i, 0)), row, row],
        flops=2 * tokens * d * (heads + 2) * HEAD,
    )


def _gap(bk, cols, bq):
    return lax.rem(lax.broadcasted_iota(jnp.int32, (bk, cols), 1), bq) - lax.broadcasted_iota(jnp.int32, (bk, cols), 0)


def _lanes(ref):
    return jnp.concatenate([ref[n : n + 1, :] for n in range(ref.shape[0])], axis=1)


def _causal(iq, bq, bk, block):
    per = bk // bq
    whole = lax.div(iq, per)
    lax.fori_loop(0, whole, lambda j, _: block(j * bk, bk, False), None)
    for m in range(per):
        pl.when(iq - whole * per == m)(lambda m=m: block(whole * bk, (m + 1) * bq, True))


def _attend_kernel(q_ref, k_ref, v_ref, o_ref, lse_ref, top_s, mix_s, gap_s, *, bq, bk, wide):
    g = q_ref.shape[0]
    cols = g * bq
    iq = pl.program_id(0)
    e = SCALE * LOG2E
    pieces = list(range(0, cols, wide))

    @pl.when(iq == 0)
    def _():
        gap_s[...] = _gap(bk, cols, bq)

    top_s[...] = jnp.full(top_s.shape, NEG, WIDE)
    mix_s[...] = jnp.zeros(mix_s.shape, WIDE)

    def block(first, size, masked):
        here = pl.ds(pl.multiple_of(first, bq), size)
        q = q_ref[...].reshape(cols, HEAD)
        scores = [_dot(k_ref[here, :], q[at : at + wide, :], 1, 1) for at in pieces]
        if masked:
            ok = gap_s[:size, :] >= first - iq * bq
        values = jnp.concatenate([v_ref[here, :].T, jnp.ones((8, size), LOW)], axis=0)
        weights, keeps = [], []
        for at, s in zip(pieces, scores):
            if masked:
                s = jnp.where(ok[:, at : at + wide], s, HIDDEN)
            old = top_s[:, at : at + wide]
            top = jnp.maximum(old, s.max(axis=0, keepdims=True))
            top_s[:, at : at + wide] = top
            weights.append(jnp.exp2((s - top) * e).astype(LOW))
            keeps.append(jnp.exp2((old - top) * e))
        for at, p, keep in zip(pieces, weights, keeps):
            mix_s[:, at : at + wide] = mix_s[:, at : at + wide] * keep + _dot(values, p, 1, 0)

    _causal(iq, bq, bk, block)
    total = mix_s[HEAD : HEAD + 1, :]
    out = mix_s[:HEAD, :] * (1 / total)
    lse = top_s[...] * SCALE + jnp.log(total)
    for n in range(g):
        o_ref[:, n * HEAD : (n + 1) * HEAD] = out[:, n * bq : (n + 1) * bq].T.astype(o_ref.dtype)
        lse_ref[n : n + 1, :] = lse[:, n * bq : (n + 1) * bq]


def attend(q, k, v, bq=512, bk=512, wide=512):
    g, tokens, _ = q.shape
    bq, bk = _fit(tokens, bq), _fit(tokens, bk)
    wide = _fit(g * bq, wide)
    return _call(
        functools.partial(_attend_kernel, bq=bq, bk=bk, wide=wide), (tokens // bq,), [q, k, v],
        [pl.BlockSpec((g, bq, HEAD), lambda i: (0, i, 0)), _whole(k), _whole(v)],
        [_new((tokens, g * HEAD)), _new((g, tokens), WIDE)],
        [_rows(bq, g * HEAD), pl.BlockSpec((g, bq), lambda i: (0, i))],
        [pltpu.VMEM((1, g * bq), WIDE), pltpu.VMEM((HEAD + 8, g * bq), WIDE), pltpu.VMEM((bk, g * bq), jnp.int32)],
        flops=4 * g * tokens * tokens * HEAD, exps=g * tokens * tokens,
    )


def _wo_kernel(o_ref, w_ref, h_ref, h2_ref, b_ref):
    h2 = (h_ref[...].astype(WIDE) + _dot(o_ref[...], w_ref[...]).astype(LOW).astype(WIDE)).astype(LOW)
    h2_ref[...] = h2
    b_ref[...] = _normed(h2)


def out_project(o, w, h):
    tokens, d = h.shape
    tm = _fit(tokens, 512)
    return _call(
        _wo_kernel, (tokens // tm,), [o, w, h], [_rows(tm, o.shape[1]), _left(w, d), _rows(tm, d)],
        [_new((tokens, d)), _new((tokens, d))], [_rows(tm, d), _rows(tm, d)], flops=2 * tokens * d * o.shape[1],
    )


def _gate_up_kernel(b_ref, wg_ref, wu_ref, g_ref, u_ref, act_ref):
    b = b_ref[...]
    g, u = _dot(b, wg_ref[...]), _dot(b, wu_ref[...])
    g_ref[...] = g
    u_ref[...] = u
    act_ref[...] = (g * lax.logistic(g) * u).astype(LOW)


def gate_up(b, w, tm=2048, tf=256):
    tokens, d = b.shape
    ff = w.shape[1] // 2
    tm, tf = _fit(tokens, tm), _fit(ff, tf)
    per = ff // tf
    tile = pl.BlockSpec((tm, tf), lambda i, j: (i, j))
    return _call(
        _gate_up_kernel, (tokens // tm, per), [b, w, w],
        [_rows(tm, d), pl.BlockSpec((d, tf), lambda i, j: (0, j)), pl.BlockSpec((d, tf), lambda i, j: (0, j + per))],
        [_new((tokens, ff), WIDE), _new((tokens, ff), WIDE), _new((tokens, ff))], [tile] * 3,
        flops=4 * tokens * d * ff, exps=tokens * ff,
    )


def _down_kernel(act_ref, w_ref, h_ref, y_ref):
    y_ref[...] = (h_ref[...].astype(WIDE) + _dot(act_ref[...], w_ref[...]).astype(LOW).astype(WIDE)).astype(LOW)


def down(act, w, h):
    tokens, d = h.shape
    tm = _fit(tokens, 512)
    return _call(
        _down_kernel, (tokens // tm,), [act, w, h], [_rows(tm, act.shape[1]), _whole(w), _rows(tm, d)],
        [_new((tokens, d))], [_rows(tm, d)], flops=2 * tokens * d * act.shape[1],
    )[0]


def _mlp_back_kernel(dy_ref, h2_ref, wg_ref, wu_ref, wd_ref, g_ref, u_ref, dgu_ref, dh_ref, db_s):
    g, u = g_ref[...], u_ref[...]
    j = pl.program_id(1)
    d_act = _dot(dy_ref[...], wd_ref[...], 1, 1).astype(LOW).astype(WIDE)
    half = lax.logistic(g)
    silu = g * half
    du = (d_act * silu).astype(LOW)
    dg = (d_act * u * (half + silu * (1 - half))).astype(LOW)
    dgu_ref[0] = dg
    dgu_ref[1] = du
    term = _dot(jnp.concatenate([dg, du], 1), jnp.concatenate([wg_ref[...], wu_ref[...]], 1), 1, 1)
    db_s[...] = jnp.where(j > 0, db_s[...], 0.0) + term

    @pl.when(j == pl.num_programs(1) - 1)
    def _():
        back = _norm_back(h2_ref[...], db_s[...].astype(LOW).astype(WIDE))
        dh_ref[...] = (dy_ref[...].astype(WIDE) + back).astype(LOW)


def mlp_back(dy, h2, w, w_down, g, u, tm=1024, tf=512):
    tokens, d = dy.shape
    ff = w.shape[1] // 2
    tm, tf = _fit(tokens, tm), _fit(ff, tf)
    per = ff // tf
    tile = pl.BlockSpec((tm, tf), lambda i, j: (i, j))
    return _call(
        _mlp_back_kernel, (tokens // tm, per), [dy, h2, w, w, w_down, g, u],
        [_rows(tm, d), _rows(tm, d), pl.BlockSpec((d, tf), lambda i, j: (0, j)), pl.BlockSpec((d, tf), lambda i, j: (0, j + per)),
         pl.BlockSpec((tf, d), lambda i, j: (j, 0)), tile, tile],
        [_new((2, tokens, ff)), _new((tokens, d))], [pl.BlockSpec((2, tm, tf), lambda i, j: (0, i, j)), _rows(tm, d)],
        [pltpu.VMEM((tm, d), WIDE)], flops=6 * tokens * d * ff, exps=tokens * ff,
    )


def _grad_kernel(a_ref, b_ref, c_ref, at_s, *, flip):
    @pl.when(pl.program_id(0) == 0)
    def _():
        at_s[...] = a_ref[...].T

    c = _dot(at_s[...], b_ref[0])
    c_ref[...] = (c.T if flip else c).astype(LOW)


def weight_grad(a, b, flip=False, tn=512):
    tokens, d = a.shape
    parts, _, n = b.shape
    tn = _fit(n, tn)
    per = n // tn
    total = parts * n
    return _call(
        functools.partial(_grad_kernel, flip=flip), (parts * per,), [a, b],
        [_whole(a), pl.BlockSpec((1, tokens, tn), lambda i: (lax.div(i, per), 0, lax.rem(i, per)))],
        [_new((total, d) if flip else (d, total))],
        [pl.BlockSpec((tn, d), lambda i: (i, 0)) if flip else pl.BlockSpec((d, tn), lambda i: (0, i))],
        [pltpu.VMEM((d, tokens), LOW)], flops=2 * tokens * d * total,
    )[0]


def _add_up(total_s, term, out_ref):
    i = pl.program_id(0)
    total_s[...] = jnp.where(i > 0, total_s[...], 0.0) + term

    @pl.when(i == pl.num_programs(0) - 1)
    def _():
        out_ref[...] = total_s[...].astype(LOW)


def _wo_back_kernel(dh_ref, w_ref, o_ref, do_ref, delta_ref, dw_ref, dw_s):
    heads, d = do_ref.shape[0], dh_ref.shape[1]
    d_out = _dot(dh_ref[...], w_ref[...], 1, 1).astype(LOW)
    _add_up(dw_s, _dot(o_ref[...].T, dh_ref[...]), dw_ref)
    along = d_out.astype(WIDE) * o_ref[...].astype(WIDE)
    for n in range(heads):
        at = slice(n * HEAD, (n + 1) * HEAD)
        do_ref[n] = d_out[:, at]
        delta_ref[n : n + 1, :] = jnp.sum(along[:, at].T, axis=0, keepdims=True)


def out_project_back(dh, w, o):
    tokens, d = dh.shape
    width = o.shape[1]
    heads = width // HEAD
    tm = _fit(tokens, 512)
    return _call(
        _wo_back_kernel, (tokens // tm,), [dh, w, o], [_rows(tm, d), _left(w, d), _rows(tm, width)],
        [_new((heads, tokens, HEAD)), _new((heads, tokens), WIDE), _new((width, d))],
        [pl.BlockSpec((heads, tm, HEAD), lambda i: (0, i, 0)), pl.BlockSpec((heads, tm), lambda i: (0, i)), pl.BlockSpec((width, d), lambda i: (0, 0))],
        [pltpu.VMEM((width, d), WIDE)], flops=4 * tokens * d * width,
    )


def _attend_back_kernel(q_ref, k_ref, v_ref, do_ref, lse_ref, delta_ref, dq_ref, dk_ref, dv_ref, dq_s, dk_s, dv_s, gap_s, *, bq, bk, wide):
    g = q_ref.shape[0]
    cols = g * bq
    iq = pl.program_id(0)
    e = SCALE * LOG2E
    pieces = list(range(0, cols, wide))

    @pl.when(iq == 0)
    def _():
        gap_s[...] = _gap(bk, cols, bq)
        dk_s[...] = jnp.zeros_like(dk_s)
        dv_s[...] = jnp.zeros_like(dv_s)

    dq_s[...] = jnp.zeros_like(dq_s)
    lses = _lanes(lse_ref) * LOG2E
    deltas = _lanes(delta_ref)

    def block(first, size, masked):
        here = pl.ds(pl.multiple_of(first, bq), size)
        q, do = q_ref[...].reshape(cols, HEAD), do_ref[...].reshape(cols, HEAD)
        qs, dos = [q[at : at + wide, :] for at in pieces], [do[at : at + wide, :] for at in pieces]
        scores = [_dot(k_ref[here, :], x, 1, 1) for x in qs]
        dps = [_dot(v_ref[here, :], x, 1, 1) for x in dos]
        if masked:
            ok = gap_s[:size, :] >= first - iq * bq
        for n, at in enumerate(pieces):
            p = jnp.exp2(scores[n] * e - lses[:, at : at + wide])
            if masked:
                p = jnp.where(ok[:, at : at + wide], p, 0.0)
            ds = (p * (dps[n] - deltas[:, at : at + wide])).astype(LOW)
            dv_s[here, :] += _dot(p.astype(LOW), dos[n], 1, 0)
            dk_s[here, :] += _dot(ds, qs[n], 1, 0)
            dq_s[:, at : at + wide] += _dot(k_ref[here, :].T, ds, 1, 0)

    _causal(iq, bq, bk, block)
    dq_ref[...] = (dq_s[...] * SCALE).T.reshape(g, bq, HEAD).astype(LOW)

    @pl.when(iq == pl.num_programs(0) - 1)
    def _():
        dk_ref[...] = (dk_s[...] * SCALE).astype(LOW)
        dv_ref[...] = dv_s[...].astype(LOW)


def attend_back(q, k, v, d_out, lse, delta, bq=256, bk=512, wide=512):
    g, tokens, _ = q.shape
    bq, bk = _fit(tokens, bq), _fit(tokens, bk)
    wide = _fit(g * bq, wide)
    block = pl.BlockSpec((g, bq, HEAD), lambda i: (0, i, 0))
    stats = pl.BlockSpec((g, bq), lambda i: (0, i))
    return _call(
        functools.partial(_attend_back_kernel, bq=bq, bk=bk, wide=wide), (tokens // bq,), [q, k, v, d_out, lse, delta],
        [block, _whole(k), _whole(v), block, stats, stats],
        [_new(q.shape), _new(k.shape), _new(v.shape)], [block, _whole(k), _whole(v)],
        [pltpu.VMEM((HEAD, g * bq), WIDE), pltpu.VMEM(k.shape, WIDE), pltpu.VMEM(v.shape, WIDE), pltpu.VMEM((bk, g * bq), jnp.int32)],
        flops=10 * g * tokens * tokens * HEAD, exps=g * tokens * tokens,
    )


def _qkv_back_kernel(dq_ref, dk_ref, dv_ref, cos_ref, sin_ref, w_ref, h_ref, dh2_ref, a_ref, dh_ref, dw_ref, dt_ref, dw_s, *, at):
    heads = dq_ref.shape[0]
    cos, sin = cos_ref[...], -sin_ref[...]
    for n in range(heads):
        dt_ref[:, n * HEAD : (n + 1) * HEAD] = _turned(dq_ref[n].astype(WIDE), cos, sin)
    dt_ref[:, heads * HEAD : (heads + 1) * HEAD] = _turned(dk_ref[...].astype(WIDE), cos, sin)
    dt_ref[:, (heads + 1) * HEAD :] = dv_ref[...]
    da = _dot(dt_ref[...], w_ref[:, at:], 1, 1).astype(LOW).astype(WIDE)
    _add_up(dw_s, _dot(a_ref[...].T, dt_ref[...]), dw_ref)
    dh_ref[...] = (dh2_ref[...].astype(WIDE) + _norm_back(h_ref[...], da)).astype(LOW)


def qkv_back(dq, dk, dv, cos, sin, w, h, dh2, a, at):
    tokens, d = h.shape
    heads = dq.shape[0]
    width = (heads + 2) * HEAD
    tm = _fit(tokens, 512)
    row = _rows(tm, HEAD)
    return _call(
        functools.partial(_qkv_back_kernel, at=at), (tokens // tm,), [dq, dk, dv, cos, sin, w, h, dh2, a],
        [pl.BlockSpec((heads, tm, HEAD), lambda i: (0, i, 0)), row, row, row, row, _whole(w), *[_rows(tm, d)] * 3],
        [_new((tokens, d)), _new((d, width))], [_rows(tm, d), pl.BlockSpec((d, width), lambda i: (0, 0))],
        [pltpu.VMEM((tm, width), LOW), pltpu.VMEM((d, width), WIDE)], flops=4 * tokens * d * width,
    )


def solution(mesh):
    def gather(w):
        return lax.all_gather(w, "dp", axis=0, tiled=True)

    def scatter(d_w):
        return lax.psum_scatter(d_w, "dp", scatter_dimension=0, tiled=True)

    tied = lambda *arrays: lax.optimization_barrier(arrays)

    def step(x, dy, wq, wk, wv, wo, w_gate, w_up, w_down):
        layers = wq.shape[0]
        h, d_h = x[0], dy[0]
        at = wo.shape[2]
        blocks = []
        for n in range(layers):
            blocks.append((
                gather(jnp.concatenate([wo[n], wq[n], wk[n], wv[n]], 1)),
                gather(jnp.concatenate([w_gate[n], w_up[n]], 1)),
                gather(w_down[n]),
            ))
        cos, sin = _angles(h.shape[0])
        kept = []
        for n in range(layers):
            near, middle, far = blocks[n]
            a, q, k, v = qkv(h, near, cos, sin, at)
            o, lse = attend(q, k, v)
            h2, b = out_project(o, near, h)
            g, u, act = gate_up(b, middle)
            kept.append((h, a, q, k, v, o, lse, h2, b, g, u, act))
            if n < layers - 1:
                h = down(act, far, h2)
        mine = [None] * layers
        late = None
        for n in reversed(range(layers)):
            near, middle, far = blocks[n]
            h, a, q, k, v, o, lse, h2, b, g, u, act = kept[n]
            dgu, dh2 = mlp_back(d_h, h2, middle, far, g, u)
            if late is not None:
                late, act, dh2 = tied(late, act, dh2)
                mine[n + 1][3] = late
            d_down, b = tied(weight_grad(d_h, act[None], flip=True), b)
            d_gu, dh2 = tied(weight_grad(b, dgu), dh2)
            d_out, delta, d_wo = out_project_back(dh2, near, o)
            d_down, d_gu, d_wo = (scatter(t) for t in (d_down, d_gu, d_wo))
            d_down, d_out = tied(d_down, d_out)
            dq, dk, dv = attend_back(q, k, v, d_out, lse, delta)
            d_gu, dq = tied(d_gu, dq)
            d_h, d_qkv = qkv_back(dq, dk, dv, cos, sin, near, h, dh2, a, at)
            d_wo, d_h = tied(d_wo, d_h)
            late = scatter(d_qkv)
            mine[n] = [d_down, d_gu, d_wo, late]
        ff = w_gate.shape[2]
        qs = wq.shape[2]
        ks = qs + wk.shape[2]
        mine = [(t[:, :qs], t[:, qs:ks], t[:, ks:], d_wo, d_gu[:, :ff], d_gu[:, ff:], d_down) for d_down, d_gu, d_wo, t in mine]
        return (d_h[None], *(jnp.stack([mine[n][i] for n in range(layers)]) for i in range(7)))

    states, cut = P(("rep", "dp"), None, None), P(None, "dp", None)
    return jax.shard_map(
        step,
        mesh=mesh,
        in_specs=(states, states) + (cut,) * 7,
        out_specs=(states,) + (P("rep", "dp", None),) * 7,
        check_vma=False,
    )
```
